32 devices in a mesh: ctx: 32 (over z, y, x, core), head: 1.
Axes of the slice: x: 2, y: 2, z: 4, core: 2. Of those that a mesh axis runs over, the one named last changes fastest.
Arguments:
- queries: bfloat16 [6144, 4096], P('ctx', 'head'), may hold values from -6 to 6
- keys: bfloat16 [6144, 1024], P('ctx', 'head'), may hold values from -6 to 6
- values: bfloat16 [6144, 1024], P('ctx', 'head'), may hold values from -6 to 6
- retrieval: int32 [32], replicated, may hold values 0 or 1
- spans: int32 [2, 32], replicated, may hold values from 64 to 4096, as said below
- out_weight: bfloat16 [4096, 4096], P(None, 'head'), may hold values from -0.09375 to 0.09375
Outputs:
- layer_out: bfloat16 [6144, 4096], P('ctx', 'head')
The draws below stay inside these ranges and needn't reach their ends.
Inputs may be any that keep to these rules, and one draw needn't show every extreme that they name: `spans`: row 0 lies within 64 to 128, row 1 within 2048 to 4096; some head has exactly 128 sink tokens and some head exactly 4096 recent tokens.
All inputs are finite; a program needn't handle non-finite values.
Results may differ from the reference program's by a relative error of at most 0.0075.
Values may be sent and summed in bfloat16 or wider, within the bound.
A program may use at most 192 MiB of HBM per device.

```python
import jax
import jax.numpy as jnp
from jax import lax

D = 4096
QH = 32
KVH = 8
HD = 128
TOK_DEV = 192
SINK = 128
WINDOW = 4096
SEQ = 6144
N_CTX = 32


def draw_queries(key, part):
    drawn = jnp.clip(jax.random.normal(jax.random.fold_in(key, 11), (SEQ, QH * HD), jnp.float32), -6.0, 6.0)
    return drawn.astype(jnp.bfloat16)


def draw_keys(key, part):
    drawn = jnp.clip(jax.random.normal(jax.random.fold_in(key, 12), (SEQ, KVH * HD), jnp.float32), -6.0, 6.0)
    return drawn.astype(jnp.bfloat16)


def draw_spans(key, part):
    sink_sizes = jax.random.randint(jax.random.fold_in(key, 21), (QH,), SINK // 2, SINK + 1)
    window_sizes = jax.random.randint(jax.random.fold_in(key, 22), (QH,), WINDOW // 2, WINDOW + 1)
    picked = jax.random.randint(jax.random.fold_in(key, 23), (2,), 0, QH)
    sink_sizes = sink_sizes.at[picked[0]].set(SINK)
    window_sizes = window_sizes.at[picked[1]].set(WINDOW)
    return jnp.stack([sink_sizes, window_sizes]).astype(jnp.int32)


def place_ends(values, stream_key, least, high):
    extent = values.shape
    place = [jax.random.randint(jax.random.fold_in(stream_key, axis), (), 0, extent[axis]) for axis in range(len(extent))]
    values = values.at[tuple(place)].set(least)
    longest = extent.index(max(extent))
    place[longest] = (place[longest] + 1) % extent[longest]
    return values.at[tuple(place)].set(high)


def block_scale(own_key, extent, split, smallest, high):
    def one(position, blocks):
        heights = jax.random.uniform(jax.random.fold_in(jax.random.fold_in(own_key, 6), position), (blocks,), jnp.float32, smallest / len(split), high / len(split))
        return jnp.repeat(jnp.exp(heights), extent[position] // blocks).reshape((-1,) + (1,) * (len(extent) - position - 1))

    loudness = one(*split[0])
    for cut in split[1:]:
        loudness = loudness * one(*cut)
    return loudness


def scatter_about(stream_key, dims, width, bound, cuts=(), held_as=jnp.bfloat16):
    drawn = jax.random.normal(stream_key, dims, jnp.float32) * width
    if len(cuts) > 0:
        drawn = block_scale(stream_key, dims, cuts, -0.22, 0.18) * drawn
    return jnp.clip(drawn, min=-bound, max=bound).astype(held_as)


def setup_inputs(seed: int = 0) -> dict:
    streams_of = jax.random.split(jax.random.key(seed), 7)
    queries = draw_queries(jax.random.fold_in(streams_of[6], 71), 0)
    keys = draw_keys(jax.random.fold_in(streams_of[6], 71), 0)
    values = scatter_about(streams_of[2], (SEQ, KVH * HD), 1.0, 6.0, ((0, 32),))
    retrieval = place_ends((jax.random.randint(streams_of[3], (QH,), 0, 2) < 1).astype(jnp.int32), jax.random.fold_in(streams_of[3], 1), 0, 1)
    spans = draw_spans(jax.random.fold_in(streams_of[6], 71), 0)
    out_weight = scatter_about(streams_of[5], (D, D), D ** -0.5, 0.09375)
    return dict(queries=queries, keys=keys, values=values, retrieval=retrieval, spans=spans, out_weight=out_weight)


def attend_block(queries_block, offset, keys, values, retrieval, spans):
    row_count = queries_block.shape[0]
    group_size = QH // KVH
    query_heads = queries_block.reshape(row_count, KVH, group_size, HD).astype(jnp.float32)
    key_heads = keys.reshape(SEQ, KVH, HD).astype(jnp.float32)
    value_heads = values.reshape(SEQ, KVH, HD).astype(jnp.float32)
    scores = jnp.einsum("qgjd,kgd->qgjk", query_heads, key_heads) * (HD ** -0.5)
    query_pos = offset + jnp.arange(row_count, dtype=jnp.int32)
    key_pos = jnp.arange(SEQ, dtype=jnp.int32)
    retrieval_heads = retrieval.reshape(KVH, group_size) > 0
    sink_sizes = spans[0].reshape(KVH, group_size)
    window_sizes = spans[1].reshape(KVH, group_size)
    gap = query_pos[:, None] - key_pos[None, :]
    reach = retrieval_heads[None, :, :, None] | (key_pos[None, None, None, :] < sink_sizes[None, :, :, None])
    reach = reach | (gap[:, None, None, :] < window_sizes[None, :, :, None])
    allowed = (gap >= 0)[:, None, None, :] & reach
    masked = jnp.where(allowed, scores, -1e30)
    peaks = jnp.max(masked, axis=-1, keepdims=True)
    weights = jnp.where(allowed, jnp.exp(masked - peaks), 0.0)
    totals = jnp.sum(weights, axis=-1)
    rounded = lax.optimization_barrier(weights.astype(jnp.bfloat16)).astype(jnp.float32)
    mixed = jnp.einsum("qgjk,kgd->qgjd", rounded, value_heads) / totals[..., None]
    return mixed.reshape(row_count, QH * HD).astype(jnp.bfloat16)


def reference(queries, keys, values, retrieval, spans, out_weight):
    blocks = queries.reshape(N_CTX, TOK_DEV, QH * HD)
    offsets = jnp.arange(N_CTX, dtype=jnp.int32) * TOK_DEV

    def one_block(pair):
        return attend_block(pair[0], pair[1], keys, values, retrieval, spans)

    attended = lax.map(one_block, (blocks, offsets)).reshape(SEQ, QH * HD)
    return jnp.dot(attended, out_weight, preferred_element_type=jnp.float32).astype(jnp.bfloat16)
```

```python
import functools

import jax
import jax.numpy as jnp
from jax import lax
from jax.experimental import pallas as pl
from jax.experimental.pallas import tpu as pltpu
from jax.sharding import PartitionSpec as P

HD = 128
LOG2E = 1.4426950408889634
MASKED = -1e30
FLOOR = -1e29
FAR = 1 << 29


def attend_kernel(group, block, first_head, meta_ref, pos_ref, q_ref, k_ref, v_ref, o_ref, stacked, peak, total, accum):
    rows = q_ref.shape[0]
    scale = (HD ** -0.5) * LOG2E
    head = first_head + pl.program_id(0) * group
    first_row = pos_ref[0]
    last_row = first_row + rows - 1
    sinks = [meta_ref[0, head + r] for r in range(group)]
    windows = [meta_ref[1, head + r] for r in range(group)]
    widest = functools.reduce(jnp.maximum, windows)
    narrowest = functools.reduce(jnp.minimum, windows)
    most_sink = functools.reduce(jnp.maximum, sinks)

    for r in range(group):
        stacked[r * rows:(r + 1) * rows, :] = q_ref[:, r * HD:(r + 1) * HD]
    peak[...] = jnp.full_like(peak, FLOOR)
    total[...] = jnp.zeros_like(total)
    accum[...] = jnp.zeros_like(accum)

    def step(index, masked):
        start = pl.multiple_of(index * block, block)
        scores = lax.dot_general(
            stacked[...], k_ref[pl.ds(start, block), :], (((1,), (1,)), ((), ())),
            preferred_element_type=jnp.float32,
        )
        if masked:
            key_pos = start + lax.broadcasted_iota(jnp.int32, (rows, block), 1)
            gap = first_row - key_pos + lax.broadcasted_iota(jnp.int32, (rows, block), 0)
            parts = []
            for r in range(group):
                allowed = (gap >= 0) & ((gap < windows[r]) | (key_pos < sinks[r]))
                parts.append(jnp.where(allowed, scores[r * rows:(r + 1) * rows], MASKED))
            scores = jnp.concatenate(parts, axis=0)
        held = peak[...]
        fresh = jnp.maximum(held, jnp.max(scores, axis=-1, keepdims=True))
        peak[...] = fresh
        shrink = jnp.exp2((held - fresh) * scale)
        weights = jnp.exp2((scores - jnp.tile(fresh, (1, block // HD))) * scale)
        added = weights[:, :HD]
        for c in range(1, block // HD):
            added = added + weights[:, c * HD:(c + 1) * HD]
        total[...] = total[...] * shrink + added
        accum[...] = accum[...] * shrink + jnp.dot(
            weights.astype(jnp.bfloat16), v_ref[pl.ds(start, block), :],
            preferred_element_type=jnp.float32,
        )

    low = jnp.maximum(first_row - widest + 1, 0) // block
    high = last_row // block + 1
    full_low = jnp.minimum((jnp.maximum(last_row - narrowest + 1, 0) + block - 1) // block, high)
    full_high = jnp.maximum((first_row + 1) // block, full_low)
    sink_blocks = jnp.minimum((most_sink + block - 1) // block, low)
    count_low = jnp.maximum(full_low - low, 0)
    masked_count = sink_blocks + count_low + (high - full_high)

    def masked_step(i, carry):
        near = i - sink_blocks
        index = jnp.where(
            near < 0, i, jnp.where(near < count_low, low + near, full_high + near - count_low)
        )
        step(index, True)
        return carry

    def full_step(i, carry):
        step(i, False)
        return carry

    lax.fori_loop(0, masked_count, masked_step, 0)
    lax.fori_loop(full_low, full_high, full_step, 0)
    mixed = accum[...] / jnp.sum(total[...], axis=-1, keepdims=True)
    for r in range(group):
        o_ref[:, r * HD:(r + 1) * HD] = mixed[r * rows:(r + 1) * rows].astype(jnp.bfloat16)


def attend(queries, gathered, meta, position, group, first_kv, kv_count):
    rows = queries.shape[0]
    seq = gathered.shape[0]
    block = 512 if seq % 512 == 0 else HD
    smem = pl.BlockSpec(memory_space=pltpu.SMEM)
    return pl.pallas_call(
        functools.partial(attend_kernel, group, block, first_kv * group),
        grid=(kv_count,),
        out_shape=jax.ShapeDtypeStruct((rows, kv_count * group * HD), jnp.bfloat16),
        in_specs=[
            smem,
            smem,
            pl.BlockSpec((rows, group * HD), lambda g: (0, first_kv + g)),
            pl.BlockSpec((seq, HD), lambda g: (0, g)),
            pl.BlockSpec((seq, HD), lambda g: (0, kv_count + g)),
        ],
        out_specs=pl.BlockSpec((rows, group * HD), lambda g: (0, g)),
        scratch_shapes=[
            pltpu.VMEM((group * rows, HD), jnp.bfloat16),
            pltpu.VMEM((group * rows, HD), jnp.float32),
            pltpu.VMEM((group * rows, HD), jnp.float32),
            pltpu.VMEM((group * rows, HD), jnp.float32),
        ],
        compiler_params=pltpu.CompilerParams(dimension_semantics=("arbitrary",)),
        cost_estimate=pl.CostEstimate(
            flops=8 * kv_count * group * rows * seq * HD,
            bytes_accessed=2 * kv_count * seq * HD * 2,
            transcendentals=kv_count * group * rows * seq,
        ),
    )(meta, position, queries, gathered, gathered)


def body(queries, keys, values, retrieval, spans, out_weight):
    rows = queries.shape[0]
    local_heads = queries.shape[1] // HD
    kv_heads = keys.shape[1] // HD
    group = local_heads // kv_heads
    head_first = lax.axis_index("head") * local_heads
    windows = jnp.where(retrieval > 0, FAR, spans[1])
    meta = lax.dynamic_slice_in_dim(jnp.stack([spans[0], windows]), head_first, local_heads, axis=1)
    position = (lax.axis_index("ctx") * rows).reshape(1).astype(jnp.int32)
    step = 2 if kv_heads % 2 == 0 else 1
    gathered = []
    for g in range(0, kv_heads, step):
        columns = slice(g * HD, (g + step) * HD)
        own = jnp.concatenate([keys[:, columns], values[:, columns]], axis=1)
        gathered.append(lax.all_gather(own, "ctx", axis=0, tiled=True))
    pieces = [
        attend(queries, gathered[i], meta, position, group, g, step)
        for i, g in enumerate(range(0, kv_heads, step))
    ]
    attended = jnp.concatenate(pieces, axis=1)
    features = lax.all_gather(attended, "head", axis=1, tiled=True)
    projected = jnp.dot(features, out_weight, preferred_element_type=jnp.float32)
    return projected.astype(jnp.bfloat16)


def solution(mesh):
    in_specs = (P("ctx", "head"), P("ctx", "head"), P("ctx", "head"), P(), P(), P(None, "head"))
    out_specs = P("ctx", "head")
    return jax.shard_map(body, mesh=mesh, in_specs=in_specs, out_specs=out_specs, check_vma=False)
```
